32 devices in a mesh: fsdp: 8 (over z, y), rep: 4 (over x, core).
Axes of the slice: x: 2, y: 2, z: 4, core: 2. Of those that a mesh axis runs over, the one named last changes fastest.
Arguments:
- hidden: bfloat16 [8192, 2048], P(('fsdp', 'rep')), may hold values from -6 to 6
- attn_gain: bfloat16 [2048], P(('fsdp', 'rep')), may hold values from 0.25 to 1.75
- w_query: bfloat16 [2048, 2048], P(('fsdp', 'rep')), as said below
- w_key: bfloat16 [2048, 512], P(('fsdp', 'rep')), as said below
- w_value: bfloat16 [2048, 512], P(('fsdp', 'rep')), may hold values from -0.125 to 0.125
- w_out: bfloat16 [2048, 2048], P(None, ('fsdp', 'rep')), may hold values from -0.125 to 0.125
Outputs:
- mixed: bfloat16 [8192, 2048], P(('fsdp', 'rep'))
The draws below stay inside these ranges and needn't reach their ends.
Inputs may be any that keep to these rules, and one draw needn't show every extreme that they name: `w_query`: entries of order 2048^(-1/2). `w_key`: entries of order 2048^(-1/2) times a factor up to twenty.
All inputs are finite; a program needn't handle non-finite values.
Results may differ from the reference program's by a relative error of at most 0.012.
The reference program's roundings to bfloat16 on the way (of `normed`, `probs` and `context`) count: a program that leaves them out, or rounds other values in their place, can miss the bound.
Values may be sent and summed in bfloat16 or wider, within the bound.
A program may use at most 64 MiB of HBM per device.

```python
import math
import jax
import jax.numpy as jnp
from jax import lax

D = 2048
HEADS = 32
KV_HEADS = 8
HD = 64
TOK_DEV = 256
TOKENS = 8192
N_FSDP = 8
N_REP = 4


def shared_base(key):
    return jax.random.normal(jax.random.fold_in(key, 7), (D, KV_HEADS, 1, HD), jnp.float32) / math.sqrt(D)


def draw_w_query(key, part):
    group = HEADS // KV_HEADS
    others = jax.random.normal(jax.random.fold_in(key, 11), (D, KV_HEADS, group, HD), jnp.float32) / math.sqrt(D)
    joined = jnp.concatenate([shared_base(key), others[:, :, 1:, :]], axis=2)
    return joined.reshape(D, HEADS * HD).astype(jnp.bfloat16)


def draw_w_key(key, part):
    noise = jax.random.normal(jax.random.fold_in(key, 13), (D, KV_HEADS * HD), jnp.float32) / math.sqrt(D)
    result = noise
    return result.astype(jnp.bfloat16)


def block_levels(stream_key, extent, shards, least, high):
    def one(dim, parts):
        draws = jax.random.uniform(jax.random.fold_in(jax.random.fold_in(stream_key, 6), dim), (parts,), jnp.float32, least / len(shards), high / len(shards))
        return jnp.repeat(jnp.exp(draws), extent[dim] // parts).reshape((-1,) + (1,) * (len(extent) - dim - 1))

    level = one(*shards[0])
    for cut in shards[1:]:
        level = level * one(*cut)
    return level


def normal_values(key, extent, spread, most, split=(), held_as=jnp.bfloat16):
    values = jax.random.normal(key, extent, jnp.float32) * spread
    if len(split) > 0:
        values = block_levels(key, extent, split, -0.22, 0.18) * values
    return jnp.clip(values, min=-most, max=most).astype(held_as)


def setup_inputs(seed: int = 0) -> dict:
    streams_of = jax.random.split(jax.random.key(seed), 7)
    return {
        "hidden": normal_values(streams_of[0], (TOKENS, D), 1.0, 6.0, ((0, 32),)),
        "attn_gain": jnp.clip(1.0 + 0.15 * jax.random.normal(streams_of[1], (D,), jnp.float32), 0.25, 1.75).astype(jnp.bfloat16),
        "w_query": draw_w_query(jax.random.fold_in(streams_of[6], 71), 0),
        "w_key": draw_w_key(jax.random.fold_in(streams_of[6], 71), 0),
        "w_value": normal_values(streams_of[4], (D, KV_HEADS * HD), D ** -0.5, 0.125, ((0, 32),)),
        "w_out": normal_values(streams_of[5], (HEADS * HD, D), (HEADS * HD) ** -0.5, 0.125, ((1, 32),)),
    }


rope_base = 500000.0
norm_eps = 1e-05

def rope_tables(tokens, head_dim):
    position = jnp.arange(tokens, dtype=jnp.float32)
    freq = rope_base ** (-(jnp.arange(head_dim // 2, dtype=jnp.float32) * 2.0) / head_dim)
    angle = position[:, None] * freq[None, :]
    cos_table = jnp.concatenate([jnp.cos(angle), jnp.cos(angle)], axis=-1)
    sin_table = jnp.concatenate([jnp.sin(angle), jnp.sin(angle)], axis=-1)
    return (cos_table, sin_table)

def rotate(tensor, cos_table, sin_table):
    half = tensor.shape[-1] // 2
    turned = jnp.concatenate([-tensor[..., half:], tensor[..., :half]], axis=-1)
    return tensor * cos_table + turned * sin_table

def reference(hidden, attn_gain, w_query, w_key, w_value, w_out):
    group = HEADS // KV_HEADS
    cos_table, sin_table = rope_tables(TOK_DEV, HD)
    causal = jnp.arange(TOK_DEV)[:, None] >= jnp.arange(TOK_DEV)[None, :]

    def one_sequence(block):
        x_float = block.astype(jnp.float32)
        inv_rms = lax.rsqrt(lax.optimization_barrier(jnp.mean(x_float * x_float, axis=-1, keepdims=True)) + norm_eps)
        normed = (x_float * inv_rms * attn_gain.astype(jnp.float32)[None, :]).astype(jnp.bfloat16)
        queries = jnp.dot(normed, w_query, preferred_element_type=jnp.float32)
        keys_raw = jnp.dot(normed, w_key, preferred_element_type=jnp.float32)
        values_raw = jnp.dot(normed, w_value, preferred_element_type=jnp.float32)
        queries = queries.reshape(TOK_DEV, KV_HEADS, group, HD)
        keys_raw = keys_raw.reshape(TOK_DEV, KV_HEADS, HD)
        values_bf = values_raw.reshape(TOK_DEV, KV_HEADS, HD).astype(jnp.bfloat16)
        rope_queries = rotate(queries, cos_table[:, None, None, :], sin_table[:, None, None, :]).astype(jnp.bfloat16)
        rope_keys = rotate(keys_raw, cos_table[:, None, :], sin_table[:, None, :]).astype(jnp.bfloat16)
        scores = jnp.einsum('qkgd,skd->kgqs', rope_queries.astype(jnp.float32), rope_keys.astype(jnp.float32)) * HD ** (-0.5)
        scores = jnp.where(causal[None, None, :, :], scores, -1e+30)
        top = lax.optimization_barrier(jnp.max(scores, axis=-1, keepdims=True))
        expo = jnp.exp(scores - top)
        probs = (expo / lax.optimization_barrier(jnp.sum(expo, axis=-1, keepdims=True))).astype(jnp.bfloat16)
        context = jnp.einsum('kgqs,skd->qkgd', probs.astype(jnp.float32), values_bf.astype(jnp.float32))
        context = context.reshape(TOK_DEV, HEADS * HD).astype(jnp.bfloat16)
        return (x_float + jnp.dot(context, w_out, preferred_element_type=jnp.float32)).astype(jnp.bfloat16)
    blocks = hidden.reshape(N_FSDP * N_REP, TOK_DEV, D)
    return lax.map(one_sequence, blocks).reshape(TOKENS, D)
```

```python
import jax
import jax.numpy as jnp
from jax import lax
from jax.sharding import PartitionSpec as P

HD = 64


rope_base = 500000.0
norm_eps = 1e-05


def rope_tables(tokens, head_dim):
    position = jnp.arange(tokens, dtype=jnp.float32)
    freq = rope_base ** (-(jnp.arange(head_dim // 2, dtype=jnp.float32) * 2.0) / head_dim)
    angle = position[:, None] * freq[None, :]
    cos_table = jnp.concatenate([jnp.cos(angle), jnp.cos(angle)], axis=-1)
    sin_table = jnp.concatenate([jnp.sin(angle), jnp.sin(angle)], axis=-1)
    return (cos_table, sin_table)


def rotate(tensor, cos_table, sin_table):
    half = tensor.shape[-1] // 2
    turned = jnp.concatenate([-tensor[..., half:], tensor[..., :half]], axis=-1)
    return tensor * cos_table + turned * sin_table


def body(hidden, attn_gain, w_query, w_key, w_value, w_out):
    tokens = hidden.shape[0]
    head_dim = HD
    width_query = w_query.shape[1]
    width_kv = w_key.shape[1]
    kv_count = width_kv // head_dim
    group = width_query // width_kv
    x_float = hidden.astype(jnp.float32)
    inv_rms = lax.rsqrt(jnp.mean(x_float * x_float, axis=-1, keepdims=True) + norm_eps)
    width_rows = w_query.shape[0]
    packed = jnp.concatenate(
        [w_query, w_key, w_value, w_out.T, jnp.broadcast_to(attn_gain[:, None], (width_rows, 128))],
        axis=1,
    )
    packed = lax.all_gather(packed, ("fsdp", "rep"), axis=0, tiled=True)
    cut_key = width_query
    cut_value = cut_key + width_kv
    cut_out = cut_value + width_kv
    cut_gain = cut_out + w_out.shape[0]
    query_piece = packed[:, :cut_key]
    key_piece = packed[:, cut_key:cut_value]
    value_piece = packed[:, cut_value:cut_out]
    out_piece = packed[:, cut_out:cut_gain]
    gain_piece = packed[:, cut_gain]
    normed = (x_float * inv_rms * gain_piece.astype(jnp.float32)[None, :]).astype(jnp.bfloat16)
    queries = jnp.dot(normed, query_piece, preferred_element_type=jnp.float32)
    keys_raw = jnp.dot(normed, key_piece, preferred_element_type=jnp.float32)
    values_raw = jnp.dot(normed, value_piece, preferred_element_type=jnp.float32)
    cos_table, sin_table = rope_tables(tokens, head_dim)
    queries = queries.reshape(tokens, kv_count, group, head_dim)
    keys_raw = keys_raw.reshape(tokens, kv_count, head_dim)
    values_bf = values_raw.reshape(tokens, kv_count, head_dim).astype(jnp.bfloat16)
    rope_queries = rotate(queries, cos_table[:, None, None, :], sin_table[:, None, None, :]).astype(
        jnp.bfloat16
    )
    rope_keys = rotate(keys_raw, cos_table[:, None, :], sin_table[:, None, :]).astype(jnp.bfloat16)
    scores = jnp.einsum(
        "qkgd,skd->kgqs", rope_queries, rope_keys, preferred_element_type=jnp.float32
    ) * head_dim ** (-0.5)
    causal = jnp.arange(tokens)[:, None] >= jnp.arange(tokens)[None, :]
    scores = jnp.where(causal[None, None, :, :], scores, -1e30)
    top = jnp.max(scores, axis=-1, keepdims=True)
    expo = jnp.exp(scores - top)
    probs = (expo / jnp.sum(expo, axis=-1, keepdims=True)).astype(jnp.bfloat16)
    context = jnp.einsum("kgqs,skd->qkgd", probs, values_bf, preferred_element_type=jnp.float32)
    context = context.reshape(tokens, width_query).astype(jnp.bfloat16)
    branch = lax.dot_general(
        context, out_piece, (((1,), (1,)), ((), ())), preferred_element_type=jnp.float32
    )
    return (x_float + branch).astype(jnp.bfloat16)


def solution(mesh):
    placed = (
        P(("fsdp", "rep"), None),
        P(("fsdp", "rep")),
        P(("fsdp", "rep"), None),
        P(("fsdp", "rep"), None),
        P(("fsdp", "rep"), None),
        P(None, ("fsdp", "rep")),
    )
    return jax.shard_map(
        body, mesh=mesh, in_specs=placed, out_specs=P(("fsdp", "rep"), None), check_vma=False
    )
```

```python
import functools

import jax
import jax.numpy as jnp
from jax import lax
from jax.experimental import pallas as pl
from jax.experimental.pallas import tpu as pltpu
from jax.sharding import PartitionSpec as P

HD = 64


rope_base = 500000.0
norm_eps = 1e-05


def rope_tables(tokens, head_dim):
    position = jnp.arange(tokens, dtype=jnp.float32)
    freq = rope_base ** (-(jnp.arange(head_dim // 2, dtype=jnp.float32) * 2.0) / head_dim)
    angle = position[:, None] * freq[None, :]
    cos_table = jnp.concatenate([jnp.cos(angle), jnp.cos(angle)], axis=-1)
    sin_table = jnp.concatenate([jnp.sin(angle), jnp.sin(angle)], axis=-1)
    return (cos_table, sin_table)


def rotate(tensor, cos_table, sin_table):
    half = tensor.shape[-1] // 2
    turned = jnp.concatenate([-tensor[..., half:], tensor[..., :half]], axis=-1)
    return tensor * cos_table + turned * sin_table


ORDERS = ((("x", "z", "y"), 2), (("y", "z", "x"), 2), (("z", "x", "y"), 1), (("z", "y", "x"), 1))
KERNEL_DEVICES = 64


def chip_grid(fsdp, rep):
    x_count = max(rep // 2, 1)
    return {"z": fsdp // x_count, "y": x_count, "x": x_count}


def column_parts(width):
    tiles = width // 128
    total = sum(weight for _, weight in ORDERS)
    cuts, seen = [0], 0
    for _, weight in ORDERS:
        seen += weight
        cuts.append((tiles * seen + total // 2) // total * 128)
    return [(order, cuts[i], cuts[i + 1] - cuts[i]) for i, (order, _) in enumerate(ORDERS)]


def gather_kernel(fsdp, rep, shard, out, send_sem, recv_sem, own_sem):
    grid = chip_grid(fsdp, rep)
    row, col = lax.axis_index("fsdp"), lax.axis_index("rep")
    here = {"z": row // grid["y"], "y": row % grid["y"], "x": col // 2}
    core = col % 2
    parts = column_parts(shard.shape[1])
    chips = fsdp * rep // 2

    def device(at, which):
        return (at["z"] * grid["y"] + at["y"], at["x"] * 2 + which)

    def slot_of(at, which):
        place = device(at, which)
        return place[0] * rep + place[1]

    def nearest(dim, step):
        p, n = here[dim], grid[dim]
        if n != 4:
            return (p + step) % n
        middle = jnp.where((p == 1) | (p == 2), 1, 0)
        high = step // 2
        low = step % 2
        low = low + middle * high * (1 - 2 * low)
        first = (1 - 2 * (p % 2)) * low
        return p + first + (2 - 4 * (p // 2)) * high

    def origin(step):
        return {
            "z": nearest("z", step // (grid["y"] * grid["x"])),
            "y": nearest("y", (step // grid["x"]) % grid["y"]),
            "x": nearest("x", step % grid["x"]),
        }

    def steps_along(dim, start):
        p, n = here[dim], grid[dim]
        if n == 2:
            return [(1 - p, p == start)]
        return [(p + 1, (p >= start) & (p + 1 < n)), (p - 1, (p <= start) & (p >= 1))]

    def moves(order, at):
        found = []
        for i, dim in enumerate(order):
            for target, go in steps_along(dim, at[dim]):
                for later in order[i + 1 :]:
                    go = go & (here[later] == at[later])
                found.append((go, device({**here, dim: target}, core)))
        found.append((None, device(here, 1 - core)))
        return found

    def copy(source, slot, step, part, move, target):
        _, begin, size = parts[part]
        piece = source if source is shard else out.at[slot]
        return pltpu.make_async_remote_copy(
            src_ref=piece.at[:, pl.ds(begin, size)],
            dst_ref=out.at[slot, :, pl.ds(begin, size)],
            send_sem=send_sem.at[step, part, move],
            recv_sem=recv_sem.at[slot, part],
            device_id=target,
            device_id_type=pl.DeviceIdType.MESH,
        )

    def each_move(source, step, part, act):
        at = origin(step)
        slot = slot_of(at, core)
        for move, (go, target) in enumerate(moves(parts[part][0], at)):
            if go is None:
                act(copy(source, slot, step, part, move, target))
            else:

                @pl.when(go)
                def _(move=move, target=target):
                    act(copy(source, slot, step, part, move, target))

    barrier = pltpu.get_barrier_semaphore()
    around = [(None, device(here, 1 - core))]
    for dim in ("z", "y", "x"):
        for target, go in steps_along(dim, here[dim]):
            around.append((go, device({**here, dim: target}, core)))
    count = 0
    for go, target in around:
        if go is None:
            pl.semaphore_signal(
                barrier, inc=1, device_id=target, device_id_type=pl.DeviceIdType.MESH
            )
            count = count + 1
        else:

            @pl.when(go)
            def _(target=target):
                pl.semaphore_signal(
                    barrier, inc=1, device_id=target, device_id_type=pl.DeviceIdType.MESH
                )

            count = count + jnp.where(go, 1, 0)
    pl.semaphore_wait(barrier, count)

    own = pltpu.make_async_copy(shard, out.at[slot_of(here, core)], own_sem)
    for part in range(len(parts)):
        each_move(shard, 0, part, lambda c: c.start())
    own.start()

    def forward(step, carry):
        at = origin(step)
        for part in range(len(parts)):
            copy(out, slot_of(at, core), step, part, 0, device(here, 1 - core)).wait_recv()
            each_move(out, step, part, lambda c: c.start())
        return carry

    lax.fori_loop(1, chips, forward, 0)
    own.wait()

    def finish(step, carry):
        at = origin(step)
        for part in range(len(parts)):
            copy(out, slot_of(at, 1 - core), step, part, 0, device(here, 1 - core)).wait_recv()
            each_move(out, step, part, lambda c: c.wait_send())
        return carry

    lax.fori_loop(0, chips, finish, 0)


def gather_rows(shard, fsdp, rep):
    rows, width = shard.shape
    grid = chip_grid(fsdp, rep)
    moves = 1 + sum(1 if n == 2 else 2 for n in grid.values())
    devices = fsdp * rep
    gathered = pl.pallas_call(
        functools.partial(gather_kernel, fsdp, rep),
        out_shape=jax.ShapeDtypeStruct((devices, rows, width), shard.dtype),
        in_specs=[pl.BlockSpec(memory_space=pltpu.VMEM)],
        out_specs=pl.BlockSpec(memory_space=pl.ANY),
        scratch_shapes=[
            pltpu.SemaphoreType.DMA((devices // 2, len(ORDERS), moves)),
            pltpu.SemaphoreType.DMA((devices, len(ORDERS))),
            pltpu.SemaphoreType.DMA,
        ],
        compiler_params=pltpu.CompilerParams(collective_id=0, has_side_effects=True),
        name="gather_rows",
    )(shard)
    return gathered.reshape(devices * rows, width)


def body(fsdp, rep, hidden, attn_gain, w_query, w_key, w_value, w_out):
    tokens = hidden.shape[0]
    head_dim = HD
    width_query = w_query.shape[1]
    width_kv = w_key.shape[1]
    kv_count = width_kv // head_dim
    group = width_query // width_kv
    x_float = hidden.astype(jnp.float32)
    inv_rms = lax.rsqrt(jnp.mean(x_float * x_float, axis=-1, keepdims=True) + norm_eps)
    width_rows = w_query.shape[0]
    packed = jnp.concatenate(
        [w_query, w_key, w_value, w_out.T, jnp.broadcast_to(attn_gain[:, None], (width_rows, 128))],
        axis=1,
    )
    x_count = rep // 2
    if rep % 2 == 0 and x_count > 1 and fsdp % x_count == 0 and fsdp * rep <= KERNEL_DEVICES:
        packed = gather_rows(packed, fsdp, rep)
    else:
        packed = lax.all_gather(packed, ("fsdp", "rep"), axis=0, tiled=True)
    cut_key = width_query
    cut_value = cut_key + width_kv
    cut_out = cut_value + width_kv
    cut_gain = cut_out + w_out.shape[0]
    query_piece = packed[:, :cut_key]
    key_piece = packed[:, cut_key:cut_value]
    value_piece = packed[:, cut_value:cut_out]
    out_piece = packed[:, cut_out:cut_gain]
    gain_piece = packed[:, cut_gain]
    normed = (x_float * inv_rms * gain_piece.astype(jnp.float32)[None, :]).astype(jnp.bfloat16)
    queries = jnp.dot(normed, query_piece, preferred_element_type=jnp.float32)
    keys_raw = jnp.dot(normed, key_piece, preferred_element_type=jnp.float32)
    values_raw = jnp.dot(normed, value_piece, preferred_element_type=jnp.float32)
    cos_table, sin_table = rope_tables(tokens, head_dim)
    queries = queries.reshape(tokens, kv_count, group, head_dim)
    keys_raw = keys_raw.reshape(tokens, kv_count, head_dim)
    values_bf = values_raw.reshape(tokens, kv_count, head_dim).astype(jnp.bfloat16)
    rope_queries = rotate(queries, cos_table[:, None, None, :], sin_table[:, None, None, :]).astype(
        jnp.bfloat16
    )
    rope_keys = rotate(keys_raw, cos_table[:, None, :], sin_table[:, None, :]).astype(jnp.bfloat16)
    scores = jnp.einsum(
        "qkgd,skd->kgqs", rope_queries, rope_keys, preferred_element_type=jnp.float32
    ) * head_dim ** (-0.5)
    causal = jnp.arange(tokens)[:, None] >= jnp.arange(tokens)[None, :]
    scores = jnp.where(causal[None, None, :, :], scores, -1e30)
    top = jnp.max(scores, axis=-1, keepdims=True)
    expo = jnp.exp(scores - top)
    probs = (expo / jnp.sum(expo, axis=-1, keepdims=True)).astype(jnp.bfloat16)
    context = jnp.einsum("kgqs,skd->qkgd", probs, values_bf, preferred_element_type=jnp.float32)
    context = context.reshape(tokens, width_query).astype(jnp.bfloat16)
    branch = lax.dot_general(
        context, out_piece, (((1,), (1,)), ((), ())), preferred_element_type=jnp.float32
    )
    return (x_float + branch).astype(jnp.bfloat16)


def solution(mesh):
    placed = (
        P(("fsdp", "rep"), None),
        P(("fsdp", "rep")),
        P(("fsdp", "rep"), None),
        P(("fsdp", "rep"), None),
        P(("fsdp", "rep"), None),
        P(None, ("fsdp", "rep")),
    )
    return jax.shard_map(
        functools.partial(body, mesh.shape["fsdp"], mesh.shape["rep"]),
        mesh=mesh,
        in_specs=placed,
        out_specs=P(("fsdp", "rep"), None),
        check_vma=False,
    )
```

```python
import functools

import jax
import jax.numpy as jnp
from jax import lax
from jax.experimental import pallas as pl
from jax.experimental.pallas import tpu as pltpu
from jax.sharding import PartitionSpec as P

HD = 64


rope_base = 500000.0
norm_eps = 1e-05


def rope_tables(tokens, head_dim):
    position = jnp.arange(tokens, dtype=jnp.float32)
    freq = rope_base ** (-(jnp.arange(head_dim // 2, dtype=jnp.float32) * 2.0) / head_dim)
    angle = position[:, None] * freq[None, :]
    cos_table = jnp.concatenate([jnp.cos(angle), jnp.cos(angle)], axis=-1)
    sin_table = jnp.concatenate([jnp.sin(angle), jnp.sin(angle)], axis=-1)
    return (cos_table, sin_table)


def rotate(tensor, cos_table, sin_table):
    half = tensor.shape[-1] // 2
    turned = jnp.concatenate([-tensor[..., half:], tensor[..., :half]], axis=-1)
    return tensor * cos_table + turned * sin_table


ORDERS = ((("x", "z", "y"), 2), (("y", "z", "x"), 2), (("z", "x", "y"), 1), (("z", "y", "x"), 1))
KERNEL_DEVICES = 64


def chip_grid(fsdp, rep):
    x_count = max(rep // 2, 1)
    return {"z": fsdp // x_count, "y": x_count, "x": x_count}


def column_parts(width):
    tiles = width // 128
    total = sum(weight for _, weight in ORDERS)
    cuts, seen = [0], 0
    for _, weight in ORDERS:
        seen += weight
        cuts.append((tiles * seen + total // 2) // total * 128)
    return [(order, cuts[i], cuts[i + 1] - cuts[i]) for i, (order, _) in enumerate(ORDERS)]


def gather_kernel(fsdp, rep, shard, out, send_sem, recv_sem, own_sem):
    grid = chip_grid(fsdp, rep)
    row, col = lax.axis_index("fsdp"), lax.axis_index("rep")
    here = {"z": row // grid["y"], "y": row % grid["y"], "x": col // 2}
    core = col % 2
    parts = column_parts(shard.shape[1])
    chips = fsdp * rep // 2

    def device(at, which):
        return (at["z"] * grid["y"] + at["y"], at["x"] * 2 + which)

    def slot_of(at, which):
        place = device(at, which)
        return place[0] * rep + place[1]

    def nearest(dim, step):
        p, n = here[dim], grid[dim]
        if n != 4:
            return (p + step) % n
        middle = jnp.where((p == 1) | (p == 2), 1, 0)
        high = step // 2
        low = step % 2
        low = low + middle * high * (1 - 2 * low)
        first = (1 - 2 * (p % 2)) * low
        return p + first + (2 - 4 * (p // 2)) * high

    def origin(step, order):
        found = {}
        for dim in order:
            found[dim] = nearest(dim, step % grid[dim])
            step = step // grid[dim]
        return found

    def steps_along(dim, start):
        p, n = here[dim], grid[dim]
        if n == 2:
            return [(1 - p, p == start)]
        return [(p + 1, (p >= start) & (p + 1 < n)), (p - 1, (p <= start) & (p >= 1))]

    def moves(order, at):
        found = []
        for i, dim in enumerate(order):
            for target, go in steps_along(dim, at[dim]):
                for later in order[i + 1 :]:
                    go = go & (here[later] == at[later])
                found.append((go, device({**here, dim: target}, core)))
        found.append((None, device(here, 1 - core)))
        return found

    def copy(source, slot, step, part, move, target):
        _, begin, size = parts[part]
        piece = source if source is shard else out.at[slot]
        return pltpu.make_async_remote_copy(
            src_ref=piece.at[:, pl.ds(begin, size)],
            dst_ref=out.at[slot, :, pl.ds(begin, size)],
            send_sem=send_sem.at[step, part, move],
            recv_sem=recv_sem.at[slot, part],
            device_id=target,
            device_id_type=pl.DeviceIdType.MESH,
        )

    def each_move(source, step, part, act):
        at = origin(step, parts[part][0])
        slot = slot_of(at, core)
        for move, (go, target) in enumerate(moves(parts[part][0], at)):
            if go is None:
                act(copy(source, slot, step, part, move, target))
            else:

                @pl.when(go)
                def _(move=move, target=target):
                    act(copy(source, slot, step, part, move, target))

    barrier = pltpu.get_barrier_semaphore()
    around = [(None, device(here, 1 - core))]
    for dim in ("z", "y", "x"):
        for target, go in steps_along(dim, here[dim]):
            around.append((go, device({**here, dim: target}, core)))
    count = 0
    for go, target in around:
        if go is None:
            pl.semaphore_signal(
                barrier, inc=1, device_id=target, device_id_type=pl.DeviceIdType.MESH
            )
            count = count + 1
        else:

            @pl.when(go)
            def _(target=target):
                pl.semaphore_signal(
                    barrier, inc=1, device_id=target, device_id_type=pl.DeviceIdType.MESH
                )

            count = count + jnp.where(go, 1, 0)
    pl.semaphore_wait(barrier, count)

    own = pltpu.make_async_copy(shard, out.at[slot_of(here, core)], own_sem)
    for part in range(len(parts)):
        each_move(shard, 0, part, lambda c: c.start())
    own.start()

    def forward(step, carry):
        for part in range(len(parts)):
            at = origin(step, parts[part][0])
            copy(out, slot_of(at, core), step, part, 0, device(here, 1 - core)).wait_recv()
            each_move(out, step, part, lambda c: c.start())
        return carry

    lax.fori_loop(1, chips, forward, 0)
    own.wait()

    def finish(step, carry):
        for part in range(len(parts)):
            at = origin(step, parts[part][0])
            copy(out, slot_of(at, 1 - core), step, part, 0, device(here, 1 - core)).wait_recv()
            each_move(out, step, part, lambda c: c.wait_send())
        return carry

    lax.fori_loop(0, chips, finish, 0)


def gather_rows(shard, fsdp, rep):
    rows, width = shard.shape
    grid = chip_grid(fsdp, rep)
    moves = 1 + sum(1 if n == 2 else 2 for n in grid.values())
    devices = fsdp * rep
    gathered = pl.pallas_call(
        functools.partial(gather_kernel, fsdp, rep),
        out_shape=jax.ShapeDtypeStruct((devices, rows, width), shard.dtype),
        in_specs=[pl.BlockSpec(memory_space=pltpu.VMEM)],
        out_specs=pl.BlockSpec(memory_space=pl.ANY),
        scratch_shapes=[
            pltpu.SemaphoreType.DMA((devices // 2, len(ORDERS), moves)),
            pltpu.SemaphoreType.DMA((devices, len(ORDERS))),
            pltpu.SemaphoreType.DMA,
        ],
        compiler_params=pltpu.CompilerParams(collective_id=0, has_side_effects=True),
        name="gather_rows",
    )(shard)
    return gathered.reshape(devices * rows, width)


def body(fsdp, rep, hidden, attn_gain, w_query, w_key, w_value, w_out):
    tokens = hidden.shape[0]
    head_dim = HD
    width_query = w_query.shape[1]
    width_kv = w_key.shape[1]
    kv_count = width_kv // head_dim
    group = width_query // width_kv
    x_float = hidden.astype(jnp.float32)
    inv_rms = lax.rsqrt(jnp.mean(x_float * x_float, axis=-1, keepdims=True) + norm_eps)
    width_rows = w_query.shape[0]
    packed = jnp.concatenate(
        [w_query, w_key, w_value, w_out.T, jnp.broadcast_to(attn_gain[:, None], (width_rows, 128))],
        axis=1,
    )
    x_count = rep // 2
    if rep % 2 == 0 and x_count > 1 and fsdp % x_count == 0 and fsdp * rep <= KERNEL_DEVICES:
        packed = gather_rows(packed, fsdp, rep)
    else:
        packed = lax.all_gather(packed, ("fsdp", "rep"), axis=0, tiled=True)
    cut_key = width_query
    cut_value = cut_key + width_kv
    cut_out = cut_value + width_kv
    cut_gain = cut_out + w_out.shape[0]
    query_piece = packed[:, :cut_key]
    key_piece = packed[:, cut_key:cut_value]
    value_piece = packed[:, cut_value:cut_out]
    out_piece = packed[:, cut_out:cut_gain]
    gain_piece = packed[:, cut_gain]
    normed = (x_float * inv_rms * gain_piece.astype(jnp.float32)[None, :]).astype(jnp.bfloat16)
    queries = jnp.dot(normed, query_piece, preferred_element_type=jnp.float32)
    keys_raw = jnp.dot(normed, key_piece, preferred_element_type=jnp.float32)
    values_raw = jnp.dot(normed, value_piece, preferred_element_type=jnp.float32)
    cos_table, sin_table = rope_tables(tokens, head_dim)
    queries = queries.reshape(tokens, kv_count, group, head_dim)
    keys_raw = keys_raw.reshape(tokens, kv_count, head_dim)
    values_bf = values_raw.reshape(tokens, kv_count, head_dim).astype(jnp.bfloat16)
    rope_queries = rotate(queries, cos_table[:, None, None, :], sin_table[:, None, None, :]).astype(
        jnp.bfloat16
    )
    rope_keys = rotate(keys_raw, cos_table[:, None, :], sin_table[:, None, :]).astype(jnp.bfloat16)
    scores = jnp.einsum(
        "qkgd,skd->kgqs", rope_queries, rope_keys, preferred_element_type=jnp.float32
    ) * head_dim ** (-0.5)
    causal = jnp.arange(tokens)[:, None] >= jnp.arange(tokens)[None, :]
    scores = jnp.where(causal[None, None, :, :], scores, -1e30)
    top = jnp.max(scores, axis=-1, keepdims=True)
    expo = jnp.exp(scores - top)
    probs = (expo / jnp.sum(expo, axis=-1, keepdims=True)).astype(jnp.bfloat16)
    context = jnp.einsum("kgqs,skd->qkgd", probs, values_bf, preferred_element_type=jnp.float32)
    context = context.reshape(tokens, width_query).astype(jnp.bfloat16)
    branch = lax.dot_general(
        context, out_piece, (((1,), (1,)), ((), ())), preferred_element_type=jnp.float32
    )
    return (x_float + branch).astype(jnp.bfloat16)


def solution(mesh):
    placed = (
        P(("fsdp", "rep"), None),
        P(("fsdp", "rep")),
        P(("fsdp", "rep"), None),
        P(("fsdp", "rep"), None),
        P(("fsdp", "rep"), None),
        P(None, ("fsdp", "rep")),
    )
    return jax.shard_map(
        functools.partial(body, mesh.shape["fsdp"], mesh.shape["rep"]),
        mesh=mesh,
        in_specs=placed,
        out_specs=P(("fsdp", "rep"), None),
        check_vma=False,
    )
```
